32 devices in a mesh: node: 8 (over z, x), expert: 4 (over y, core).
Axes of the slice: x: 2, y: 2, z: 4, core: 2. Of those that a mesh axis runs over, the one named last changes fastest.
Arguments:
- tokens: bfloat16 [16384, 1024], P(('node', 'expert')), may hold values from -6 to 6
- queries: bfloat16 [16384, 1024], P(('node', 'expert')), may hold values from -6 to 6
- keys: bfloat16 [16384, 1024], P(('node', 'expert')), may hold values from -6 to 6
- values: bfloat16 [16384, 1024], P(('node', 'expert')), may hold values from -12 to 12
- neighbours: int32 [128, 8], P(('node', 'expert')), may hold values from 0 to 127, as said below
- live_bits: int32 [128, 8], P(('node', 'expert')), may hold values from 0 to 1, as said below
- out_proj: bfloat16 [1024, 1024], replicated, may hold values from -0.1875 to 0.1875
- norm_gain: float32 [1024], replicated, may hold values from 0.5 to 1.5
- router: bfloat16 [1024, 32], replicated, may hold values from -0.1875 to 0.1875
- expert: int32 [16384], P(('node', 'expert')), may hold values from 0 to 31, as said below
- slot: int32 [16384], P(('node', 'expert')), may hold values from 0 to 31, as said below
- w_up: bfloat16 [32, 1024, 4096], P(('node', 'expert')), may hold values from -0.1875 to 0.1875
- w_down: bfloat16 [32, 4096, 1024], P(('node', 'expert')), may hold values from -0.09375 to 0.09375
Outputs:
- layer_out: bfloat16 [16384, 1024], P(('node', 'expert'))
The draws below stay inside these ranges and needn't reach their ends.
Inputs may be any that keep to these rules, and one draw needn't show every extreme that they name: Tile g is held by device g // 4 in node-major order. neighbours[g, 0] is g itself; every listed tile is held by g's device or by the device one step before or after it along node with the same expert index (wrapping around); entry 1 is always one step before and entry 2 one step after. `live_bits`: entry 0 of every row is 1. Within the 512 tokens of one device, no two tokens share both expert and slot; some expert takes all 32 slots of every device. See expert: pairs (expert, slot) are distinct within one device's tokens.
All inputs are finite; a program needn't handle non-finite values.
Results may differ from the reference program's by a relative error of at most 0.0049.
Values may be sent and summed in bfloat16 or wider, within the bound.
A program may use at most 192 MiB of HBM per device.

```python
import jax
import jax.numpy as jnp
from jax import lax

D = 1024
HEADS = 16
HEAD_DIM = 64
FF = 4096
TILE = 128
NB = 8
TOK_DEV = 512
EXPERTS = 32
CAP = 32
TOKENS = 16384
TILES = 128
N_NODE = 8
N_EXPERT = 4
DEVICES = 32


def query_key_pair(key):
    base_query = jnp.clip(jax.random.normal(jax.random.fold_in(key, 31), (TOKENS, D), jnp.float32) * 1.3, -6.0, 6.0)
    base_key = jnp.clip(jax.random.normal(jax.random.fold_in(key, 32), (TOKENS, D), jnp.float32) * 1.3, -6.0, 6.0)
    return (base_query, base_key)


def draw_queries(key, part):
    return query_key_pair(key)[0].astype(jnp.bfloat16)


def draw_keys(key, part):
    return query_key_pair(key)[1].astype(jnp.bfloat16)


def draw_neighbours(key, part):
    tile_count = TOKENS // TILE
    tiles_dev = TOK_DEV // TILE
    tile_ids = jnp.arange(tile_count, dtype=jnp.int32)
    device_of = tile_ids // tiles_dev
    node_of = device_of // N_EXPERT
    column_of = device_of % N_EXPERT
    steps = jax.random.randint(key, (tile_count, NB), -1, 2, jnp.int32)
    steps = steps.at[:, 0].set(0).at[:, 1].set(-1).at[:, 2].set(1)
    picks = jax.random.randint(jax.random.fold_in(key, 1), (tile_count, NB), 0, tiles_dev, jnp.int32)
    other_device = (node_of[:, None] + steps + N_NODE) % N_NODE * N_EXPERT + column_of[:, None]
    listed = other_device * tiles_dev + picks
    listed = listed.at[:, 0].set(tile_ids)
    return listed.astype(jnp.int32)


def draw_live_bits(key, part):
    tile_count = TOKENS // TILE
    drawn = jax.random.randint(jax.random.fold_in(key, 5), (tile_count, NB), 0, 4, jnp.int32)
    bits = jnp.where(drawn > 0, 1, 0).astype(jnp.int32)
    return bits.at[:, 0].set(1)


def route_cells(key):
    block_count = TOKENS // TOK_DEV
    cell_count = EXPERTS * CAP
    noise = jax.random.randint(jax.random.fold_in(key, 21), (block_count, cell_count), 0, 2 ** 18, jnp.int32)
    heat = jax.random.randint(jax.random.fold_in(key, 22), (EXPERTS,), 0, 2 ** 18, jnp.int32)
    hottest = jax.random.randint(jax.random.fold_in(key, 23), (), 0, EXPERTS, jnp.int32)
    owner_of = jnp.arange(cell_count, dtype=jnp.int32) // CAP
    scores = noise + heat[owner_of][None, :] + jnp.where(owner_of == hottest, 2 ** 19, 0)[None, :]
    ranked = jnp.argsort(-scores, axis=1, stable=True)[:, :TOK_DEV]
    return ranked.reshape(TOKENS).astype(jnp.int32)


def draw_expert(key, part):
    return (route_cells(key) // CAP).astype(jnp.int32)


def draw_slot(key, part):
    return (route_cells(key) % CAP).astype(jnp.int32)


def block_scale(key, extent, split, least, top_value):
    def one(position, parts):
        draws = jax.random.uniform(jax.random.fold_in(jax.random.fold_in(key, 6), position), (parts,), jnp.float32, least / len(split), top_value / len(split))
        return jnp.repeat(jnp.exp(draws), extent[position] // parts).reshape((-1,) + (1,) * (len(extent) - position - 1))

    loudness = one(*split[0])
    for cut in split[1:]:
        loudness = loudness * one(*cut)
    return loudness


def scatter_about(rng, extent, deviation, bound, pieces=(), held_as=jnp.bfloat16):
    values = jax.random.normal(rng, extent, jnp.float32) * deviation
    if len(pieces) > 0:
        values = block_scale(rng, extent, pieces, -0.22, 0.18) * values
    return jnp.clip(values, min=-bound, max=bound).astype(held_as)


def setup_inputs(seed: int = 0) -> dict:
    seeds = jax.random.split(jax.random.key(seed), 14)
    tokens = scatter_about(seeds[0], (TOKENS, D), 1.0, 6.0, ((0, 32),))
    queries = draw_queries(jax.random.fold_in(seeds[13], 71), 0)
    keys = draw_keys(jax.random.fold_in(seeds[13], 71), 0)
    values = scatter_about(seeds[3], (TOKENS, D), 2.0, 12.0, ((0, 32),))
    neighbours = draw_neighbours(jax.random.fold_in(seeds[13], 71), 0)
    live_bits = draw_live_bits(jax.random.fold_in(seeds[13], 71), 0)
    out_proj = scatter_about(seeds[6], (D, D), D ** -0.5, 0.1875)
    norm_gain = jnp.clip(1.0 + 0.1 * jax.random.normal(seeds[7], (D,), jnp.float32), 0.5, 1.5)
    router = scatter_about(seeds[8], (D, EXPERTS), D ** -0.5, 0.1875)
    expert = draw_expert(jax.random.fold_in(seeds[13], 71), 0)
    slot = draw_slot(jax.random.fold_in(seeds[13], 71), 0)
    w_up = scatter_about(seeds[11], (EXPERTS, D, FF), D ** -0.5, 0.1875, ((0, 32),))
    w_down = scatter_about(seeds[12], (EXPERTS, FF, D), FF ** -0.5, 0.09375, ((0, 32),))
    return dict(tokens=tokens, queries=queries, keys=keys, values=values, neighbours=neighbours, live_bits=live_bits, out_proj=out_proj, norm_gain=norm_gain, router=router, expert=expert, slot=slot, w_up=w_up, w_down=w_down)


score_scale = 0.125

def attend_tile(packed, key_tiles, value_tiles):
    query_tile, listed, bits = packed
    near_keys = key_tiles[listed].reshape(NB * TILE, HEADS, HEAD_DIM).astype(jnp.float32)
    near_values = value_tiles[listed].reshape(NB * TILE, HEADS, HEAD_DIM).astype(jnp.float32)
    query_heads = query_tile.reshape(TILE, HEADS, HEAD_DIM).astype(jnp.float32)
    scores = jnp.einsum('qhd,khd->hqk', query_heads, near_keys) * score_scale
    visible = jnp.repeat(bits, TILE) > 0
    masked = jnp.where(visible[None, None, :], scores, -jnp.inf)
    peak = lax.optimization_barrier(jnp.max(masked, axis=-1, keepdims=True))
    weights = jnp.exp(masked - peak)
    weights = (weights / lax.optimization_barrier(jnp.sum(weights, axis=-1, keepdims=True))).astype(jnp.bfloat16)
    mixed = jnp.einsum('hqk,khd->qhd', weights.astype(jnp.float32), near_values)
    return mixed.reshape(TILE, D).astype(jnp.bfloat16)

def reference(tokens, queries, keys, values, neighbours, live_bits, out_proj, norm_gain, router, expert, slot, w_up, w_down):
    key_tiles = keys.reshape(TILES, TILE, D)
    value_tiles = values.reshape(TILES, TILE, D)
    query_tiles = queries.reshape(TILES, TILE, D)
    attn = lax.map(lambda packed: attend_tile(packed, key_tiles, value_tiles), (query_tiles, neighbours, live_bits))
    attn = attn.reshape(TOKENS, D)
    hidden = tokens.astype(jnp.float32) + jnp.dot(attn, out_proj, preferred_element_type=jnp.float32)
    spread = lax.optimization_barrier(jnp.mean(hidden * hidden, axis=-1, keepdims=True))
    normed = (hidden * lax.rsqrt(spread + 1e-06) * norm_gain.astype(jnp.float32)[None, :]).astype(jnp.bfloat16)
    logits = jnp.dot(normed, router, preferred_element_type=jnp.float32)
    columns = jnp.arange(EXPERTS, dtype=jnp.int32)
    chosen = lax.optimization_barrier(jnp.sum(jnp.where(columns[None, :] == expert[:, None], logits, 0.0), axis=-1))
    gate = jax.nn.sigmoid(chosen)
    positions = jnp.arange(TOKENS, dtype=jnp.int32)
    target = expert * (DEVICES * CAP) + positions // TOK_DEV * CAP + slot
    table = jnp.full((EXPERTS * DEVICES * CAP,), TOKENS, jnp.int32).at[target].set(positions)
    padded = jnp.concatenate([normed, jnp.zeros((1, D), jnp.bfloat16)], axis=0)

    def run_expert(packed):
        index_rows, up_matrix, down_matrix = packed
        token_rows = padded[index_rows]
        lifted = jnp.dot(token_rows, up_matrix, preferred_element_type=jnp.float32)
        lifted = jax.nn.gelu(lifted, approximate=True).astype(jnp.bfloat16)
        return jnp.dot(lifted, down_matrix, preferred_element_type=jnp.float32).astype(jnp.bfloat16)
    results = lax.map(run_expert, (table.reshape(EXPERTS, DEVICES * CAP), w_up, w_down))
    expert_out = results.reshape(EXPERTS * DEVICES * CAP, D)[target]
    layer_out = hidden + gate[:, None] * expert_out.astype(jnp.float32)
    return layer_out.astype(jnp.bfloat16)
```

```python
import functools

import jax
import jax.numpy as jnp
from jax import lax
from jax.experimental import pallas as pl
from jax.experimental.pallas import tpu as pltpu
from jax.sharding import PartitionSpec as P

D = 1024
HEADS = 16
HEAD_DIM = 64
TILE = 128
NB = 8


score_scale = 0.125


CHUNKS = 4
HIDE = -1e30


def attention_kernel(
    nodes,
    position_ref,
    bias_ref,
    query_ref,
    key_ref,
    value_ref,
    token_ref,
    proj_ref,
    gain_ref,
    hidden_ref,
    normed_ref,
    *scratch,
):
    key_windows, value_windows = scratch[:CHUNKS], scratch[CHUNKS : 2 * CHUNKS]
    own_sem, x_send, x_recv, z_send, z_recv, attn_ref = scratch[2 * CHUNKS :]
    node = lax.axis_index("node")
    odd = node % 2
    partner = node + 1 - 2 * odd
    onward = (node + 2 - 4 * odd + nodes) % nodes
    behind = (node - 2 + 4 * odd + nodes) % nodes
    tiles = key_windows[0].shape[0] // 3
    width = key_windows[0].shape[2]
    barrier = pltpu.get_barrier_semaphore()
    for other in (partner, onward, behind):
        pl.semaphore_signal(
            barrier, inc=1, device_id={"node": other}, device_id_type=pl.DeviceIdType.MESH
        )
    pl.semaphore_wait(barrier, 3)
    own, first, second = [], [], []
    for c in range(CHUNKS):
        columns = pl.ds(c * width, width)
        for s, (source, window) in enumerate(
            ((key_ref, key_windows[c]), (value_ref, value_windows[c]))
        ):
            block = source.at[:, :, columns]
            own.append(
                pltpu.make_async_copy(block, window.at[pl.ds(0, tiles)], own_sem.at[2 * c + s])
            )
            first.append(
                pltpu.make_async_remote_copy(
                    src_ref=block,
                    dst_ref=window.at[pl.ds(tiles, tiles)],
                    send_sem=x_send.at[2 * c + s],
                    recv_sem=x_recv.at[2 * c + s],
                    device_id={"node": partner},
                    device_id_type=pl.DeviceIdType.MESH,
                )
            )
            second.append(
                pltpu.make_async_remote_copy(
                    src_ref=window.at[pl.ds(tiles, tiles)],
                    dst_ref=window.at[pl.ds(2 * tiles, tiles)],
                    send_sem=z_send.at[2 * c + s],
                    recv_sem=z_recv.at[2 * c + s],
                    device_id={"node": onward},
                    device_id_type=pl.DeviceIdType.MESH,
                )
            )
    for copy in first:
        copy.start()
    for copy in own:
        copy.start()
    hidden_ref[...] = token_ref[...].astype(jnp.float32)
    heads = width // HEAD_DIM
    lane_head = lax.broadcasted_iota(jnp.int32, (TILE, width), 1) // HEAD_DIM

    def relay(c):
        for s in range(2):
            first[2 * c + s].wait_recv()
            second[2 * c + s].start()

    def attend(c):
        def one_tile(t, carry):
            rows = pl.ds(pl.multiple_of(t * TILE, TILE), TILE)
            query = query_ref[rows, c * width : (c + 1) * width] * jnp.bfloat16(score_scale)
            near_keys = jnp.concatenate(
                [key_windows[c][position_ref[t, j]] for j in range(NB)], axis=0
            )
            near_values = jnp.concatenate(
                [value_windows[c][position_ref[t, j]] for j in range(NB)], axis=0
            )
            bias = bias_ref[t]
            mixed = jnp.zeros((TILE, width), jnp.float32)
            for h in range(heads):
                mine = jnp.where(lane_head == h, query, jnp.zeros_like(query))
                scores = lax.dot_general(
                    mine,
                    near_keys,
                    (((1,), (1,)), ((), ())),
                    preferred_element_type=jnp.float32,
                )
                scores = scores + bias
                peak = jnp.max(scores, axis=-1, keepdims=True)
                weights = jnp.exp(scores - peak)
                share = 1.0 / jnp.sum(weights, axis=-1, keepdims=True)
                weights = (weights * share).astype(jnp.bfloat16)
                out = jnp.dot(weights, near_values, preferred_element_type=jnp.float32)
                mixed = jnp.where(lane_head == h, out, mixed)
            attn_ref[rows, :] = mixed.astype(jnp.bfloat16)
            return carry

        lax.fori_loop(0, tiles, one_tile, 0)

        def project(t, carry):
            rows = pl.ds(pl.multiple_of(t * TILE, TILE), TILE)
            hidden_ref[rows, :] += jnp.dot(
                attn_ref[rows, :],
                proj_ref[c * width : (c + 1) * width, :],
                preferred_element_type=jnp.float32,
            )
            return carry

        lax.fori_loop(0, tiles, project, 0)

    relay(0)
    for c in range(CHUNKS):
        if c + 1 < CHUNKS:
            relay(c + 1)
        for s in range(2):
            own[2 * c + s].wait()
            second[2 * c + s].wait_recv()
        attend(c)

    def finish(t, carry):
        rows = pl.ds(pl.multiple_of(t * TILE, TILE), TILE)
        hidden = hidden_ref[rows, :]
        spread = jnp.mean(hidden * hidden, axis=-1, keepdims=True)
        normed = hidden * lax.rsqrt(spread + 1e-06) * gain_ref[...]
        normed_ref[rows, :] = normed.astype(jnp.bfloat16)
        return carry

    lax.fori_loop(0, tiles, finish, 0)
    for copy in first + second:
        copy.wait_send()


def attention_block(tokens, queries, keys, values, position, live_bits, out_proj, norm_gain):
    tok_dev = tokens.shape[0]
    tiles = tok_dev // TILE
    width = D // CHUNKS
    bias = jnp.where(jnp.repeat(live_bits, TILE, axis=1) > 0, 0.0, HIDE).astype(jnp.float32)
    window = pltpu.VMEM((3 * tiles, TILE, width), jnp.bfloat16)
    sems = pltpu.SemaphoreType.DMA((2 * CHUNKS,))
    vmem = pl.BlockSpec(memory_space=pltpu.VMEM)
    return pl.pallas_call(
        functools.partial(attention_kernel, lax.axis_size("node")),
        out_shape=(
            jax.ShapeDtypeStruct((tok_dev, D), jnp.float32),
            jax.ShapeDtypeStruct((tok_dev, D), jnp.bfloat16),
        ),
        in_specs=[
            pl.BlockSpec(memory_space=pltpu.SMEM),
            vmem,
            vmem,
            pl.BlockSpec(memory_space=pl.ANY),
            pl.BlockSpec(memory_space=pl.ANY),
            vmem,
            vmem,
            vmem,
        ],
        out_specs=(vmem, vmem),
        scratch_shapes=[window] * (2 * CHUNKS)
        + [sems] * 5
        + [pltpu.VMEM((tok_dev, width), jnp.bfloat16)],
        compiler_params=pltpu.CompilerParams(
            collective_id=0, has_side_effects=True, vmem_limit_bytes=48 * 1024 * 1024
        ),
    )(
        position,
        bias.reshape(tiles, 1, NB * TILE),
        queries,
        keys.reshape(tiles, TILE, D),
        values.reshape(tiles, TILE, D),
        tokens,
        out_proj,
        norm_gain.reshape(1, D),
    )


def shards(
    tokens,
    queries,
    keys,
    values,
    neighbours,
    live_bits,
    out_proj,
    norm_gain,
    router,
    expert,
    slot,
    w_up,
    w_down,
):
    tok_dev = tokens.shape[0]
    tiles_dev = tok_dev // TILE
    experts = router.shape[1]
    cap = 2 * tok_dev // experts
    my_node = lax.axis_index("node")
    column_count = lax.axis_size("expert")
    owner_node = neighbours // tiles_dev // column_count
    partner = my_node + 1 - 2 * (my_node % 2)
    block_of = jnp.where(owner_node == my_node, 0, jnp.where(owner_node == partner, 1, 2))
    position = block_of * tiles_dev + neighbours % tiles_dev
    hidden, normed = attention_block(
        tokens, queries, keys, values, position, live_bits, out_proj, norm_gain
    )
    logits = jnp.dot(normed, router, preferred_element_type=jnp.float32)
    columns = lax.iota(jnp.int32, experts)
    chosen = jnp.sum(jnp.where(columns[None, :] == expert[:, None], logits, 0.0), axis=-1)
    gate = jax.nn.sigmoid(chosen)
    slot_cell = expert * cap + slot
    one_hot = (lax.iota(jnp.int32, experts * cap)[:, None] == slot_cell[None, :]).astype(
        jnp.bfloat16
    )
    outgoing = jnp.dot(one_hot, normed, preferred_element_type=jnp.float32).astype(jnp.bfloat16)
    up_matrix = w_up[0]
    down_matrix = w_down[0]
    block = lax.all_to_all(
        outgoing.reshape(experts, 1, cap, D),
        ("node", "expert"),
        split_axis=0,
        concat_axis=1,
        tiled=True,
    )
    token_rows = block.reshape(-1, D)
    lifted = jnp.dot(token_rows, up_matrix, preferred_element_type=jnp.float32)
    lifted = jax.nn.gelu(lifted, approximate=True).astype(jnp.bfloat16)
    result = jnp.dot(lifted, down_matrix, preferred_element_type=jnp.float32).astype(jnp.bfloat16)
    returned = lax.all_to_all(
        result.reshape(block.shape), ("node", "expert"), split_axis=1, concat_axis=0, tiled=True
    )
    flat_back = returned.reshape(experts * cap, D)
    expert_out = jnp.einsum("ct,cd->td", one_hot, flat_back, preferred_element_type=jnp.float32)
    layer_out = hidden + gate[:, None] * expert_out
    return layer_out.astype(jnp.bfloat16)


def solution(mesh):
    in_specs = (
        P(("node", "expert"), None),
        P(("node", "expert"), None),
        P(("node", "expert"), None),
        P(("node", "expert"), None),
        P(("node", "expert"), None),
        P(("node", "expert"), None),
        P(),
        P(),
        P(),
        P(("node", "expert")),
        P(("node", "expert")),
        P(("node", "expert"), None, None),
        P(("node", "expert"), None, None),
    )
    out_specs = P(("node", "expert"), None)
    return jax.shard_map(shards, mesh=mesh, in_specs=in_specs, out_specs=out_specs, check_vma=False)
```

```python
import functools

import jax
import jax.numpy as jnp
from jax import lax
from jax.experimental import pallas as pl
from jax.experimental.pallas import tpu as pltpu
from jax.sharding import PartitionSpec as P

D = 1024
HEADS = 16
HEAD_DIM = 64
TILE = 128
NB = 8


score_scale = 0.125


CHUNKS = 4
HIDE = -1e30
STACK = 2


def attention_kernel(
    nodes,
    position_ref,
    bias_ref,
    query_hbm,
    key_ref,
    value_ref,
    token_hbm,
    proj_hbm,
    gain_ref,
    hidden_ref,
    normed_ref,
    *scratch,
):
    key_windows, value_windows = scratch[:CHUNKS], scratch[CHUNKS : 2 * CHUNKS]
    own_sem, x_send, x_recv, z_send, z_recv, attn_ref = scratch[2 * CHUNKS : 2 * CHUNKS + 6]
    query_ref, token_ref, proj_ref, load_sem = scratch[2 * CHUNKS + 6 :]
    token_load = pltpu.make_async_copy(token_hbm, token_ref, load_sem.at[0])
    query_load = pltpu.make_async_copy(query_hbm, query_ref, load_sem.at[1])
    proj_load = pltpu.make_async_copy(proj_hbm, proj_ref, load_sem.at[2])
    node = lax.axis_index("node")
    odd = node % 2
    partner = node + 1 - 2 * odd
    onward = (node + 2 - 4 * odd + nodes) % nodes
    behind = (node - 2 + 4 * odd + nodes) % nodes
    tiles = key_windows[0].shape[0] // 3
    width = key_windows[0].shape[2]
    barrier = pltpu.get_barrier_semaphore()
    for other in (partner, onward, behind):
        pl.semaphore_signal(
            barrier, inc=1, device_id={"node": other}, device_id_type=pl.DeviceIdType.MESH
        )
    pl.semaphore_wait(barrier, 3)
    own, first, second = [], [], []
    for c in range(CHUNKS):
        columns = pl.ds(c * width, width)
        for s, (source, window) in enumerate(
            ((key_ref, key_windows[c]), (value_ref, value_windows[c]))
        ):
            block = source.at[:, :, columns]
            own.append(
                pltpu.make_async_copy(block, window.at[pl.ds(0, tiles)], own_sem.at[2 * c + s])
            )
            first.append(
                pltpu.make_async_remote_copy(
                    src_ref=block,
                    dst_ref=window.at[pl.ds(tiles, tiles)],
                    send_sem=x_send.at[2 * c + s],
                    recv_sem=x_recv.at[2 * c + s],
                    device_id={"node": partner},
                    device_id_type=pl.DeviceIdType.MESH,
                )
            )
            second.append(
                pltpu.make_async_remote_copy(
                    src_ref=window.at[pl.ds(tiles, tiles)],
                    dst_ref=window.at[pl.ds(2 * tiles, tiles)],
                    send_sem=z_send.at[2 * c + s],
                    recv_sem=z_recv.at[2 * c + s],
                    device_id={"node": onward},
                    device_id_type=pl.DeviceIdType.MESH,
                )
            )
    for copy in first:
        copy.start()
    for copy in own + [token_load, query_load, proj_load]:
        copy.start()
    token_load.wait()
    hidden_ref[...] = token_ref[...].astype(jnp.float32)
    heads = width // HEAD_DIM
    lane_head = lax.broadcasted_iota(jnp.int32, (TILE, width), 1) // HEAD_DIM

    def relay(c):
        for s in range(2):
            first[2 * c + s].wait_recv()
            second[2 * c + s].start()

    def attend(c):
        def one_tile(t, carry):
            rows = pl.ds(pl.multiple_of(t * TILE, TILE), TILE)
            query = query_ref[rows, c * width : (c + 1) * width] * jnp.bfloat16(score_scale)
            near_keys = jnp.concatenate(
                [key_windows[c][position_ref[t, j]] for j in range(NB)], axis=0
            )
            near_values = jnp.concatenate(
                [value_windows[c][position_ref[t, j]] for j in range(NB)], axis=0
            )
            bias = bias_ref[t]
            mixed = jnp.zeros((TILE, width), jnp.float32)
            for h in range(0, heads, STACK):
                mine = jnp.concatenate(
                    [
                        jnp.where(lane_head == h + i, query, jnp.zeros_like(query))
                        for i in range(STACK)
                    ],
                    axis=0,
                )
                scores = lax.dot_general(
                    mine,
                    near_keys,
                    (((1,), (1,)), ((), ())),
                    preferred_element_type=jnp.float32,
                )
                scores = scores + bias
                peak = jnp.max(scores, axis=-1, keepdims=True)
                weights = jnp.exp(scores - peak)
                share = 1.0 / jnp.sum(weights, axis=-1, keepdims=True)
                weights = (weights * share).astype(jnp.bfloat16)
                out = jnp.dot(weights, near_values, preferred_element_type=jnp.float32)
                for i in range(STACK):
                    mixed = jnp.where(lane_head == h + i, out[i * TILE : (i + 1) * TILE], mixed)
            attn_ref[rows, :] = mixed.astype(jnp.bfloat16)
            return carry

        lax.fori_loop(0, tiles, one_tile, 0)

        def project(t, carry):
            rows = pl.ds(pl.multiple_of(t * TILE, TILE), TILE)
            hidden_ref[rows, :] += jnp.dot(
                attn_ref[rows, :],
                proj_ref[c * width : (c + 1) * width, :],
                preferred_element_type=jnp.float32,
            )
            return carry

        lax.fori_loop(0, tiles, project, 0)

    query_load.wait()
    proj_load.wait()
    relay(0)
    for c in range(CHUNKS):
        if c + 1 < CHUNKS:
            relay(c + 1)
        for s in range(2):
            own[2 * c + s].wait()
            second[2 * c + s].wait_recv()
        attend(c)

    def finish(t, carry):
        rows = pl.ds(pl.multiple_of(t * TILE, TILE), TILE)
        hidden = hidden_ref[rows, :]
        spread = jnp.mean(hidden * hidden, axis=-1, keepdims=True)
        normed = hidden * lax.rsqrt(spread + 1e-06) * gain_ref[...]
        normed_ref[rows, :] = normed.astype(jnp.bfloat16)
        return carry

    lax.fori_loop(0, tiles, finish, 0)
    for copy in first + second:
        copy.wait_send()


def attention_block(tokens, queries, keys, values, position, live_bits, out_proj, norm_gain):
    tok_dev = tokens.shape[0]
    tiles = tok_dev // TILE
    width = D // CHUNKS
    bias = jnp.where(jnp.repeat(live_bits, TILE, axis=1) > 0, 0.0, HIDE).astype(jnp.float32)
    window = pltpu.VMEM((3 * tiles, TILE, width), jnp.bfloat16)
    sems = pltpu.SemaphoreType.DMA((2 * CHUNKS,))
    vmem = pl.BlockSpec(memory_space=pltpu.VMEM)
    anywhere = pl.BlockSpec(memory_space=pl.ANY)
    return pl.pallas_call(
        functools.partial(attention_kernel, lax.axis_size("node")),
        out_shape=(
            jax.ShapeDtypeStruct((tok_dev, D), jnp.float32),
            jax.ShapeDtypeStruct((tok_dev, D), jnp.bfloat16),
        ),
        in_specs=[
            pl.BlockSpec(memory_space=pltpu.SMEM),
            vmem,
            anywhere,
            anywhere,
            anywhere,
            anywhere,
            anywhere,
            vmem,
        ],
        out_specs=(vmem, vmem),
        scratch_shapes=[window] * (2 * CHUNKS)
        + [sems] * 5
        + [
            pltpu.VMEM((tok_dev, width), jnp.bfloat16),
            pltpu.VMEM((tok_dev, D), jnp.bfloat16),
            pltpu.VMEM((tok_dev, D), jnp.bfloat16),
            pltpu.VMEM((D, D), jnp.bfloat16),
            pltpu.SemaphoreType.DMA((3,)),
        ],
        compiler_params=pltpu.CompilerParams(
            collective_id=0, has_side_effects=True, vmem_limit_bytes=62 * 1024 * 1024
        ),
    )(
        position,
        bias.reshape(tiles, 1, NB * TILE),
        queries,
        keys.reshape(tiles, TILE, D),
        values.reshape(tiles, TILE, D),
        tokens,
        out_proj,
        norm_gain.reshape(1, D),
    )


GROUPS = 4
SPAN = 512


def expert_kernel(
    nodes, columns, outgoing_ref, up_ref, down_ref, back_ref, *scratch
):
    (
        rows_ref,
        result_ref,
        up_held,
        down_held,
        total_ref,
        weight_sem,
        own_sem,
        there_send,
        there_recv,
        back_send,
        back_recv,
    ) = scratch
    devices = nodes * columns
    cap = outgoing_ref.shape[1]
    members = devices // GROUPS
    me = lax.axis_index("node") * columns + lax.axis_index("expert")
    up_copy = pltpu.make_async_copy(up_ref.at[0], up_held, weight_sem.at[0])
    down_copy = pltpu.make_async_copy(down_ref.at[0], down_held, weight_sem.at[1])

    def place(device):
        return {"node": device // columns, "expert": device % columns}

    barrier = pltpu.get_barrier_semaphore()

    def greet(k, carry):
        pl.semaphore_signal(
            barrier,
            inc=1,
            device_id=place((me + k) % devices),
            device_id_type=pl.DeviceIdType.MESH,
        )
        return carry

    lax.fori_loop(1, devices, greet, 0)
    pl.semaphore_wait(barrier, devices - 1)

    def block(g, j):
        return pl.ds(pl.multiple_of(j * cap, cap), cap)

    def there(i):
        g, j = i // members, i % members
        target = (me + g + GROUPS * j) % devices
        return pltpu.make_async_remote_copy(
            src_ref=outgoing_ref.at[target],
            dst_ref=rows_ref.at[g, block(g, j)],
            send_sem=there_send.at[i],
            recv_sem=there_recv.at[i],
            device_id=place(target),
            device_id_type=pl.DeviceIdType.MESH,
        )

    def back(i):
        g, j = i // members, i % members
        target = (me + devices - g - GROUPS * j) % devices
        return pltpu.make_async_remote_copy(
            src_ref=result_ref.at[g, block(g, j)],
            dst_ref=back_ref.at[me],
            send_sem=back_send.at[i],
            recv_sem=back_recv.at[i],
            device_id=place(target),
            device_id_type=pl.DeviceIdType.MESH,
        )

    def back_from(i):
        g, j = i // members, i % members
        source = (me + g + GROUPS * j) % devices
        return pltpu.make_async_remote_copy(
            src_ref=result_ref.at[g, block(g, j)],
            dst_ref=back_ref.at[source],
            send_sem=back_send.at[i],
            recv_sem=back_recv.at[i],
            device_id=place(source),
            device_id_type=pl.DeviceIdType.MESH,
        )

    def each(lower, upper, act):
        def step(i, carry):
            act(i)
            return carry

        lax.fori_loop(lower, upper, step, 0)

    each(1, devices, lambda i: there(i).start())
    up_copy.start()
    down_copy.start()
    own_rows = pltpu.make_async_copy(
        outgoing_ref.at[me], rows_ref.at[0, pl.ds(0, cap)], own_sem.at[0]
    )
    own_rows.start()
    own_back = pltpu.make_async_copy(
        result_ref.at[0, pl.ds(0, cap)], back_ref.at[me], own_sem.at[1]
    )
    spans = up_held.shape[1] // SPAN
    for g in range(GROUPS):
        first = max(g * members, 1)
        each(first, (g + 1) * members, lambda i: there(i).wait_recv())
        if g == 0:
            own_rows.wait()
            up_copy.wait()
            down_copy.wait()

        def span(f, carry, g=g):
            part = pl.ds(pl.multiple_of(f * SPAN, SPAN), SPAN)
            lifted = jnp.dot(rows_ref[g], up_held[:, part], preferred_element_type=jnp.float32)
            lifted = jax.nn.gelu(lifted, approximate=True).astype(jnp.bfloat16)
            total_ref[...] += jnp.dot(
                lifted, down_held[part, :], preferred_element_type=jnp.float32
            )
            return carry

        total_ref[...] = jnp.zeros_like(total_ref)
        lax.fori_loop(0, spans, span, 0)
        result_ref[g] = total_ref[...].astype(jnp.bfloat16)
        if g == 0:
            own_back.start()
        each(first, (g + 1) * members, lambda i: back(i).start())
    own_back.wait()
    each(1, devices, lambda i: there(i).wait_send())
    each(1, devices, lambda i: back(i).wait_send())
    each(1, devices, lambda i: back_from(i).wait_recv())


def expert_exchange(outgoing, w_up, w_down):
    devices, cap, _ = outgoing.shape
    hidden_units = w_up.shape[2]
    rows = devices // GROUPS * cap
    anywhere = pl.BlockSpec(memory_space=pl.ANY)
    sems = pltpu.SemaphoreType.DMA((devices,))
    pair = pltpu.SemaphoreType.DMA((2,))
    return pl.pallas_call(
        functools.partial(expert_kernel, lax.axis_size("node"), lax.axis_size("expert")),
        out_shape=jax.ShapeDtypeStruct(outgoing.shape, jnp.bfloat16),
        in_specs=[anywhere] * 3,
        out_specs=anywhere,
        scratch_shapes=[
            pltpu.VMEM((GROUPS, rows, D), jnp.bfloat16),
            pltpu.VMEM((GROUPS, rows, D), jnp.bfloat16),
            pltpu.VMEM((D, hidden_units), jnp.bfloat16),
            pltpu.VMEM((hidden_units, D), jnp.bfloat16),
            pltpu.VMEM((rows, D), jnp.float32),
            pair,
            pair,
            sems,
            sems,
            sems,
            sems,
        ],
        compiler_params=pltpu.CompilerParams(
            collective_id=1, has_side_effects=True, vmem_limit_bytes=62 * 1024 * 1024
        ),
    )(outgoing, w_up, w_down)


def exchange_by_blocks(outgoing, w_up, w_down):
    experts, cap, _ = outgoing.shape
    block = lax.all_to_all(
        outgoing.reshape(experts, 1, cap, D),
        ("node", "expert"),
        split_axis=0,
        concat_axis=1,
        tiled=True,
    )
    token_rows = block.reshape(-1, D)
    lifted = jnp.dot(token_rows, w_up[0], preferred_element_type=jnp.float32)
    lifted = jax.nn.gelu(lifted, approximate=True).astype(jnp.bfloat16)
    result = jnp.dot(lifted, w_down[0], preferred_element_type=jnp.float32).astype(jnp.bfloat16)
    return lax.all_to_all(
        result.reshape(block.shape), ("node", "expert"), split_axis=1, concat_axis=0, tiled=True
    )


def shards(
    tokens,
    queries,
    keys,
    values,
    neighbours,
    live_bits,
    out_proj,
    norm_gain,
    router,
    expert,
    slot,
    w_up,
    w_down,
):
    tok_dev = tokens.shape[0]
    tiles_dev = tok_dev // TILE
    experts = router.shape[1]
    cap = 2 * tok_dev // experts
    my_node = lax.axis_index("node")
    column_count = lax.axis_size("expert")
    owner_node = neighbours // tiles_dev // column_count
    partner = my_node + 1 - 2 * (my_node % 2)
    block_of = jnp.where(owner_node == my_node, 0, jnp.where(owner_node == partner, 1, 2))
    position = block_of * tiles_dev + neighbours % tiles_dev
    hidden, normed = attention_block(
        tokens, queries, keys, values, position, live_bits, out_proj, norm_gain
    )
    logits = jnp.dot(normed, router, preferred_element_type=jnp.float32)
    columns = lax.iota(jnp.int32, experts)
    chosen = jnp.sum(jnp.where(columns[None, :] == expert[:, None], logits, 0.0), axis=-1)
    gate = jax.nn.sigmoid(chosen)
    slot_cell = expert * cap + slot
    one_hot = (lax.iota(jnp.int32, experts * cap)[:, None] == slot_cell[None, :]).astype(
        jnp.bfloat16
    )
    outgoing = jnp.dot(one_hot, normed, preferred_element_type=jnp.float32).astype(jnp.bfloat16)
    exchange = exchange_by_blocks if cap % 16 else expert_exchange
    returned = exchange(outgoing.reshape(experts, cap, D), w_up, w_down)
    flat_back = returned.reshape(experts * cap, D)
    expert_out = jnp.einsum("ct,cd->td", one_hot, flat_back, preferred_element_type=jnp.float32)
    layer_out = hidden + gate[:, None] * expert_out
    return layer_out.astype(jnp.bfloat16)


def solution(mesh):
    in_specs = (
        P(("node", "expert"), None),
        P(("node", "expert"), None),
        P(("node", "expert"), None),
        P(("node", "expert"), None),
        P(("node", "expert"), None),
        P(("node", "expert"), None),
        P(),
        P(),
        P(),
        P(("node", "expert")),
        P(("node", "expert")),
        P(("node", "expert"), None, None),
        P(("node", "expert"), None, None),
    )
    out_specs = P(("node", "expert"), None)
    return jax.shard_map(shards, mesh=mesh, in_specs=in_specs, out_specs=out_specs, check_vma=False)
```
